32 devices in a mesh: pair: 4 (over y, x), aux: 8 (over z, core).
Axes of the slice: x: 2, y: 2, z: 4, core: 2. Of those that a mesh axis runs over, the one named last changes fastest.
Arguments:
- same_panels: bfloat16 [32, 2, 112, 59904], P('aux', None, None, 'pair'), may hold values from -1 to 1
- opposite_panels: bfloat16 [32, 2, 112, 59904], P('aux', None, None, 'pair'), may hold values from -1 to 1
- same_amplitudes: bfloat16 [32, 112, 112], replicated, may hold values from -2 to 2
- opposite_amplitudes: bfloat16 [32, 112, 112], replicated, may hold values from -2 to 2
- same_energies: float32 [32, 2, 112], replicated, may hold values from 0.5 to 3
- opposite_energies: float32 [32, 2, 112], replicated, may hold values from 0.5 to 3
- same_ranks: int32 [32], replicated, may hold values from 48 to 112
- opposite_ranks: int32 [32], replicated, may hold values from 48 to 112
Outputs:
- same_residual: float32 [32, 112, 112], P('pair', 'aux')
- opposite_residual: float32 [32, 112, 112], P('pair', 'aux')
The draws below stay inside these ranges and needn't reach their ends.
Inputs may be any that keep to these rules, and one draw needn't show every extreme that they name: `same_ranks`: slots at or beyond a pair's rank are padding. `opposite_ranks`: slots at or beyond a pair's rank are padding.
All inputs are finite; a program needn't handle non-finite values.
Results may differ from the reference program's by a relative error of at most 0.0013.
Values may be sent and summed in bfloat16 or wider, within the bound.
No kernel may reach another device: no remote copies, remote signals or barrier semaphores. Data moves between devices by JAX's collectives and lax.ppermute only.
A program may use at most 128 MiB of HBM per device.

```python
import math
import jax
import jax.numpy as jnp
from jax import lax

R = 112
NAUX = 59904
PAIRS = 32


def with_ends(entries, key, least, top_value):
    dims = entries.shape
    index_at = [jax.random.randint(jax.random.fold_in(key, axis), (), 0, dims[axis]) for axis in range(len(dims))]
    entries = entries.at[tuple(index_at)].set(least)
    longest = dims.index(max(dims))
    index_at[longest] = (index_at[longest] + 1) % dims[longest]
    return entries.at[tuple(index_at)].set(top_value)


def steps_of(own_key, extent, shards, smallest, largest):
    def one(position, parts):
        heights = jax.random.uniform(jax.random.fold_in(jax.random.fold_in(own_key, 6), position), (parts,), jnp.float32, smallest / len(shards), largest / len(shards))
        return jnp.repeat(jnp.exp(heights), extent[position] // parts).reshape((-1,) + (1,) * (len(extent) - position - 1))

    level = one(*shards[0])
    for cut in shards[1:]:
        level = level * one(*cut)
    return level


def bell_draw(stream_key, shape, deviation, limit, pieces=(), kind=jnp.bfloat16):
    factor_of = steps_of(stream_key, shape, pieces, -0.22, 0.18) if pieces else 1.0
    values = jax.random.normal(stream_key, shape, jnp.float32) * deviation * factor_of
    return jnp.minimum(jnp.maximum(values, -limit), limit).astype(kind)


def setup_inputs(seed: int = 0) -> dict:
    arg_keys = jax.random.split(jax.random.key(seed), 9)
    same_panels = bell_draw(arg_keys[0], (PAIRS, 2, R, NAUX), (NAUX ** -0.25), 1.0, ((0, 8), (3, 4)))
    opposite_panels = bell_draw(arg_keys[1], (PAIRS, 2, R, NAUX), (NAUX ** -0.25), 1.0, ((0, 8), (3, 4)))
    same_amplitudes = bell_draw(arg_keys[2], (PAIRS, R, R), 0.15, 2.0)
    opposite_amplitudes = bell_draw(arg_keys[3], (PAIRS, R, R), 0.15, 2.0)
    same_energies = jnp.clip(jnp.exp(jax.random.uniform(arg_keys[4], (PAIRS, 2, R), jnp.float32, math.log(0.5), math.log(3.0))), 0.5, 3.0)
    opposite_energies = jnp.clip(jnp.exp(jax.random.uniform(arg_keys[5], (PAIRS, 2, R), jnp.float32, math.log(0.5), math.log(3.0))), 0.5, 3.0)
    same_ranks = with_ends(jax.random.randint(arg_keys[6], (PAIRS,), R * 3 // 7, R + 1), jax.random.fold_in(arg_keys[6], 1), R * 3 // 7, R).astype(jnp.int32)
    opposite_ranks = with_ends(jax.random.randint(arg_keys[7], (PAIRS,), R * 3 // 7, R + 1), jax.random.fold_in(arg_keys[7], 1), R * 3 // 7, R).astype(jnp.int32)
    return dict(same_panels=same_panels, opposite_panels=opposite_panels, same_amplitudes=same_amplitudes, opposite_amplitudes=opposite_amplitudes, same_energies=same_energies, opposite_energies=opposite_energies, same_ranks=same_ranks, opposite_ranks=opposite_ranks)


def slot_mask(ranks):
    slots = jnp.arange(R, dtype=jnp.int32)
    return (slots[None, :] < ranks[:, None]).astype(jnp.float32)


def masked_amplitudes(amplitudes, keep):
    outer = keep[:, :, None] * keep[:, None, :]
    return (amplitudes.astype(jnp.float32) * outer).astype(jnp.bfloat16)


def dressing_rows(panels, masked):
    def one_pair(items):
        panel, amplitude = items
        mixed = jnp.dot(amplitude, panel[1], preferred_element_type=jnp.float32)
        return jnp.sum(panel[0].astype(jnp.float32) * mixed, axis=0)
    return lax.map(one_pair, (panels, masked))


def residual_rows(panels, masked, energies, keep, coupling):
    def one_pair(items):
        panel, amplitude, energy, mask_row = items
        exchange = jnp.dot(panel[0], panel[1].T, preferred_element_type=jnp.float32)
        scaled = (panel[0].astype(jnp.float32) * coupling[None, :]).astype(jnp.bfloat16)
        coulomb = jnp.dot(scaled, panel[1].T, preferred_element_type=jnp.float32)
        diagonal = (energy[0][:, None] + energy[1][None, :]) * amplitude.astype(jnp.float32)
        return (exchange + coulomb + diagonal) * (mask_row[:, None] * mask_row[None, :])
    return lax.map(one_pair, (panels, masked, energies, keep))


def reference(same_panels, opposite_panels, same_amplitudes, opposite_amplitudes, same_energies, opposite_energies, same_ranks, opposite_ranks):
    same_keep = slot_mask(same_ranks)
    opposite_keep = slot_mask(opposite_ranks)
    same_masked = masked_amplitudes(same_amplitudes, same_keep)
    opposite_masked = masked_amplitudes(opposite_amplitudes, opposite_keep)
    coupling = jnp.sum(dressing_rows(same_panels, same_masked), axis=0) + jnp.sum(dressing_rows(opposite_panels, opposite_masked), axis=0)
    same_residual = residual_rows(same_panels, same_masked, same_energies, same_keep, coupling)
    opposite_residual = residual_rows(opposite_panels, opposite_masked, opposite_energies, opposite_keep, coupling)
    return same_residual, opposite_residual
```

```python
import functools

import jax
import jax.numpy as jnp
from jax import lax
from jax.experimental import pallas as pl
from jax.experimental.pallas import tpu as pltpu
from jax.sharding import PartitionSpec as P

STEP = 256
SMALL = 8 * 1024 * 1024
ROW_BY_ROW = (((1,), (1,)), ((), ()))

ANYWHERE = pl.BlockSpec(memory_space=pltpu.HBM)
SCALARS = pl.BlockSpec(memory_space=pltpu.SMEM)
ON_CHIP = pl.BlockSpec(memory_space=pltpu.VMEM)


def pieces(total, step):
    return [(at, min(step, total - at)) for at in range(0, total, step)]


def call(kernel, outs, ins, scratch=(), flops=0, name=None):
    placed = [
        value if spec is not ON_CHIP else pltpu.with_memory_space_constraint(value, pltpu.VMEM)
        for spec, value in ins
    ]
    return pl.pallas_call(
        kernel,
        out_shape=tuple(pltpu.VMEM(shape, dtype) for shape, dtype in outs),
        in_specs=[spec for spec, _ in ins],
        out_specs=(ON_CHIP,) * len(outs),
        scratch_shapes=list(scratch),
        compiler_params=pltpu.CompilerParams(vmem_limit_bytes=SMALL),
        cost_estimate=pl.CostEstimate(flops=flops, bytes_accessed=0, transcendentals=0),
        name=name,
    )(*placed)


def mask(rank, slots):
    rows = lax.broadcasted_iota(jnp.int32, (slots, slots), 0) < rank
    columns = lax.broadcasted_iota(jnp.int32, (slots, slots), 1) < rank
    return jnp.logical_and(rows, columns)


def dressing_kernel(
    places,
    same_ranks,
    opposite_ranks,
    same_ref,
    opposite_ref,
    same_amp_ref,
    opposite_amp_ref,
    same_energy_ref,
    opposite_energy_ref,
    same_held,
    opposite_held,
    coupling_ref,
    base_ref,
    amp,
    energy,
    masked,
    total,
    panel_sem,
    small_sem,
):
    count, _, slots, functions = same_held.shape
    start = places[0]
    sources = (same_ref, opposite_ref)
    held = (same_held, opposite_held)
    small_copies = [
        pltpu.make_async_copy(
            source.at[pl.ds(start, count)], target.at[spin], small_sem.at[place, spin]
        )
        for place, (target, pair_of) in enumerate(
            (
                (amp, (same_amp_ref, opposite_amp_ref)),
                (energy, (same_energy_ref, opposite_energy_ref)),
            )
        )
        for spin, source in enumerate(pair_of)
    ]
    for copy in small_copies:
        copy.start()
    for spin in range(2):
        for pair in range(count):
            pltpu.make_async_copy(
                sources[spin].at[pair], held[spin].at[pair], panel_sem.at[spin, pair]
            ).start()
    for copy in small_copies:
        copy.wait()
    share = jnp.where(places[1] == 0, 1.0, 0.0)
    for spin, ranks in enumerate((same_ranks, opposite_ranks)):
        for pair in range(count):
            keep = mask(ranks[start + pair], slots)
            value = jnp.where(keep, amp[spin, pair].astype(jnp.float32), 0.0)
            masked[spin, pair] = value.astype(jnp.bfloat16)
            gaps = energy[spin, pair]
            first = jnp.broadcast_to(gaps[0:1], (slots, slots)).T
            base_ref[spin, pair] = (first + gaps[1:2]) * value * share
    total[...] = jnp.zeros_like(total)
    for spin in range(2):
        panels = held[spin]

        @pl.loop(0, count)
        def _(pair):
            pltpu.make_async_copy(
                sources[spin].at[pair], panels.at[pair], panel_sem.at[spin, pair]
            ).wait()
            weights = masked[spin, pair]
            exchange = jnp.zeros((slots, slots), jnp.float32)
            for at, size in pieces(functions, STEP):
                left = panels[pair, 0, :, at : at + size]
                right = panels[pair, 1, :, at : at + size]
                mixed = jnp.dot(weights, right, preferred_element_type=jnp.float32)
                part = left.astype(jnp.float32) * mixed
                total[:, at : at + size] += jnp.sum(part.reshape(slots // 8, 8, size), axis=0)
                exchange += lax.dot_general(
                    left, right, ROW_BY_ROW, preferred_element_type=jnp.float32
                )
            base_ref[spin, pair] += exchange

    coupling_ref[...] = jnp.sum(total[...], axis=0, keepdims=True)


def coulomb_kernel(
    places,
    same_ranks,
    opposite_ranks,
    same_held,
    opposite_held,
    base_ref,
    *rest,
    partners,
    group,
):
    couplings, outs = rest[:partners], rest[partners:-3]
    coupling, finished, whole = rest[-3:]
    count, _, slots, functions = same_held.shape
    start, pair_index, owner = places[0], places[1], places[2]
    coupling[...] = functools.reduce(jnp.add, [ref[...] for ref in couplings])
    for spin, (panels, ranks) in enumerate(
        ((same_held, same_ranks), (opposite_held, opposite_ranks))
    ):

        @pl.loop(0, count)
        def _(pair):
            summed = jnp.zeros((slots, slots), jnp.float32)
            for at, size in pieces(functions, STEP):
                left = panels[pair, 0, :, at : at + size].astype(jnp.float32)
                scaled = (left * coupling[:, at : at + size]).astype(jnp.bfloat16)
                right = panels[pair, 1, :, at : at + size]
                summed += lax.dot_general(
                    scaled, right, ROW_BY_ROW, preferred_element_type=jnp.float32
                )
            keep = mask(ranks[start + pair], slots)
            finished[spin, pair] = jnp.where(keep, summed + base_ref[spin, pair], 0.0)

    for spin in range(2):
        for pair in range(count):
            whole[:, spin * count + pair, :] = finished[spin, pair]
    rows = slots // len(outs)
    for k, out in enumerate(outs):
        at = (pair_index ^ k ^ owner) * rows
        out[...] = whole[pl.ds(at, rows)]


def add_kernel(same_held, opposite_held, *refs):
    refs[-1][...] = functools.reduce(jnp.add, [ref[...] for ref in refs[:-1]])


def gather_kernel(places, *rest, partners, group):
    parts, outs = rest[:partners], rest[partners:-1]
    summed = rest[-1]
    summed[...] = functools.reduce(jnp.add, [ref[...] for ref in parts])
    rows = outs[0].shape[0]
    for k, out in enumerate(outs):
        out[...] = summed[pl.ds(lax.rem(places[3] + k, group) * rows, rows)]


def last_kernel(places, *rest, group):
    parts, outs = rest[:group], rest[group:]
    count = parts[0].shape[1] // 2
    values = [ref[...] for ref in parts]
    for j in range(group):
        value = values[0]
        for k in range(1, group):
            value = jnp.where(lax.rem(j + k, group) == places[3], values[k], value)
        for spin, out in enumerate(outs):
            out[:, j * count : (j + 1) * count, :] = value[:, spin * count : (spin + 1) * count, :]


def body(
    same_panels,
    opposite_panels,
    same_amplitudes,
    opposite_amplitudes,
    same_energies,
    opposite_energies,
    same_ranks,
    opposite_ranks,
):
    count, _, slots, functions = same_panels.shape
    pairs, auxes = lax.axis_size("pair"), lax.axis_size("aux")
    pair_index, aux_index = lax.axis_index("pair"), lax.axis_index("aux")
    group = auxes // pairs
    rows = slots // auxes
    f32 = jnp.float32
    places = jnp.stack(
        [aux_index * count, pair_index, aux_index // group, aux_index % group]
    ).astype(jnp.int32)
    same_held, opposite_held, coupling, base = call(
        dressing_kernel,
        (
            (same_panels.shape, same_panels.dtype),
            (opposite_panels.shape, opposite_panels.dtype),
            ((1, functions), f32),
            ((2, count, slots, slots), f32),
        ),
        [(SCALARS, places), (SCALARS, same_ranks), (SCALARS, opposite_ranks)]
        + [
            (ANYWHERE, value)
            for value in (
                same_panels,
                opposite_panels,
                same_amplitudes,
                opposite_amplitudes,
                same_energies,
                opposite_energies,
            )
        ],
        [
            pltpu.VMEM((2, count, slots, slots), jnp.bfloat16),
            pltpu.VMEM((2, count, 2, slots), f32),
            pltpu.VMEM((2, count, slots, slots), jnp.bfloat16),
            pltpu.VMEM((8, functions), f32),
            pltpu.SemaphoreType.DMA((2, count)),
            pltpu.SemaphoreType.DMA((2, 2)),
        ],
        flops=8 * count * slots * slots * functions,
        name="dressing",
    )

    def swapped(value, k):
        return lax.ppermute(value, "aux", [(i, i ^ k) for i in range(auxes)])

    (coupling,) = call(
        add_kernel,
        (((1, functions), f32),),
        [
            (ON_CHIP, value)
            for value in (same_held, opposite_held, coupling, swapped(coupling, 1))
        ],
        name="chip_sum",
    )
    couplings = [coupling] + [swapped(coupling, k) for k in range(2, auxes, 2)]
    leaving = call(
        functools.partial(coulomb_kernel, partners=len(couplings), group=group),
        (((group * rows, 2 * count, slots), f32),) * pairs,
        [(SCALARS, places), (SCALARS, same_ranks), (SCALARS, opposite_ranks)]
        + [(ON_CHIP, value) for value in (same_held, opposite_held, base, *couplings)],
        [
            pltpu.VMEM((1, functions), f32),
            pltpu.VMEM((2, count, slots, slots), f32),
            pltpu.VMEM((slots, 2 * count, slots), f32),
        ],
        flops=4 * count * slots * slots * functions,
        name="coulomb",
    )
    parts = [leaving[0]] + [
        lax.ppermute(leaving[k], "pair", [(i, i ^ k) for i in range(pairs)])
        for k in range(1, pairs)
    ]
    moving = call(
        functools.partial(gather_kernel, partners=pairs, group=group),
        (((rows, 2 * count, slots), f32),) * group,
        [(SCALARS, places)] + [(ON_CHIP, value) for value in parts],
        [pltpu.VMEM((group * rows, 2 * count, slots), f32)],
        name="pair_sum",
    )
    arrived = []
    for k in range(group):
        moves = [
            (
                p * auxes + q,
                (q // group) * auxes + group * (p ^ (q // group)) + (q % group + k) % group,
            )
            for p in range(pairs)
            for q in range(auxes)
        ]
        arrived.append(lax.ppermute(moving[k], ("pair", "aux"), moves))
    outs = pl.pallas_call(
        functools.partial(last_kernel, group=group),
        out_shape=(jax.ShapeDtypeStruct((rows, group * count, slots), f32),) * 2,
        in_specs=[SCALARS] + [ON_CHIP] * group,
        out_specs=(ON_CHIP, ON_CHIP),
        name="residual_rows",
    )(places, *(pltpu.with_memory_space_constraint(value, pltpu.VMEM) for value in arrived))
    return tuple(out.transpose(1, 0, 2) for out in outs)


def solution(mesh):
    placed = (
        P("aux", None, None, "pair"),
        P("aux", None, None, "pair"),
        P(),
        P(),
        P(),
        P(),
        P(),
        P(),
    )
    return jax.shard_map(
        body,
        mesh=mesh,
        in_specs=placed,
        out_specs=(P("pair", "aux", None), P("pair", "aux", None)),
        check_vma=False,
    )
```

```python
import functools

import jax
import jax.numpy as jnp
from jax import lax
from jax.experimental import pallas as pl
from jax.experimental.pallas import tpu as pltpu
from jax.sharding import PartitionSpec as P

STEP = 256
AHEAD = 3
PARTS = 1
LANES = 128
ROWS = 16
FINE = 16
SMALL = 8 * 1024 * 1024
ROW_BY_ROW = (((1,), (1,)), ((), ()))

ANYWHERE = pl.BlockSpec(memory_space=pltpu.HBM)
SCALARS = pl.BlockSpec(memory_space=pltpu.SMEM)
ON_CHIP = pl.BlockSpec(memory_space=pltpu.VMEM)


def pieces(total, step):
    return [(at, min(step, total - at)) for at in range(0, total, step)]


def column_spans(functions):
    if functions % LANES:
        return [(0, functions)]
    length = -(-functions // (PARTS * STEP)) * STEP
    return pieces(functions, length)


def call(kernel, outs, ins, scratch=(), flops=0, name=None):
    placed = [
        value if spec is not ON_CHIP else pltpu.with_memory_space_constraint(value, pltpu.VMEM)
        for spec, value in ins
    ]
    return pl.pallas_call(
        kernel,
        out_shape=tuple(pltpu.VMEM(shape, dtype) for shape, dtype in outs),
        in_specs=[spec for spec, _ in ins],
        out_specs=(ON_CHIP,) * len(outs),
        scratch_shapes=list(scratch),
        compiler_params=pltpu.CompilerParams(vmem_limit_bytes=SMALL),
        cost_estimate=pl.CostEstimate(flops=flops, bytes_accessed=0, transcendentals=0),
        name=name,
    )(*placed)


def mask(rank, slots):
    rows = lax.broadcasted_iota(jnp.int32, (slots, slots), 0) < rank
    columns = lax.broadcasted_iota(jnp.int32, (slots, slots), 1) < rank
    return jnp.logical_and(rows, columns)


def row_cuts(slots):
    least = slots * 3 // 7 // ROWS * ROWS
    return list(range(least, slots, ROWS)) + [slots] if least else [slots]


def copy_bounds(slots):
    least = row_cuts(slots)[0]
    return [(0, least)] + [(low, low + FINE) for low in range(least, slots, FINE)]


def on_rows(rank, cuts, work):
    for place, rows in enumerate(cuts):
        fits = rank <= rows
        if place == len(cuts) - 1:
            fits = True
        if place:
            fits = jnp.logical_and(rank > cuts[place - 1], fits)
        pl.when(fits)(functools.partial(work, rows))


def add_exchange(held, base_ref, pair, rows):
    exchange = jnp.zeros((rows, rows), jnp.float32)
    for at, size in pieces(held.shape[-1], STEP):
        exchange += lax.dot_general(
            held[pair, 0, :rows, at : at + size],
            held[pair, 1, :rows, at : at + size],
            ROW_BY_ROW,
            preferred_element_type=jnp.float32,
        )
    base_ref[pair, :rows, :rows] += exchange


def exchange_kernel(same_ranks, opposite_ranks, held, base_in, base_ref, ranks, *, early):
    both, _, slots, _ = held.shape
    count = both // 2
    start = lax.axis_index("aux") * count
    for pair in range(count):
        ranks[pair] = same_ranks[start + pair]
        ranks[count + pair] = opposite_ranks[start + pair]
    base_ref[...] = base_in[...]

    @pl.loop(early, both)
    def _(pair):
        on_rows(
            ranks[pair], row_cuts(slots), functools.partial(add_exchange, held, base_ref, pair)
        )


def dressing_kernel(
    same_ranks,
    opposite_ranks,
    same_ref,
    opposite_ref,
    same_amp_ref,
    opposite_amp_ref,
    same_energy_ref,
    opposite_energy_ref,
    held,
    coupling_ref,
    base_ref,
    amp,
    energy,
    masked,
    total,
    ranks,
    panel_sem,
    small_sem,
    *,
    early,
):
    both, _, slots, functions = held.shape
    count = both // 2
    start = lax.axis_index("aux") * count
    sources = (same_ref, opposite_ref)
    cuts = row_cuts(slots)
    bounds = copy_bounds(slots)
    spans = column_spans(functions)
    parts = len(spans)
    for pair in range(count):
        ranks[pair] = same_ranks[start + pair]
        ranks[count + pair] = opposite_ranks[start + pair]

    def copies(source, pair, part, do):
        at, size = spans[part]
        for place, (low, high) in enumerate(bounds):

            def one(place=place, low=low, high=high):
                do(
                    pltpu.make_async_copy(
                        source.at[lax.rem(pair, count), :, low:high, pl.ds(at, size)],
                        held.at[pair, :, low:high, pl.ds(at, size)],
                        panel_sem.at[pair, part, place],
                    )
                )

            if place:
                pl.when(ranks[pair] > low)(one)
            else:
                one()

    def begin(pair, part):
        for spin, source in enumerate(sources):

            @pl.when(jnp.logical_and(pair >= spin * count, pair < (spin + 1) * count))
            def _():
                copies(source, pair, part, lambda copy: copy.start())

    begin(jnp.int32(0), 0)
    small_copies = [
        pltpu.make_async_copy(
            source.at[pl.ds(start, count)],
            target.at[pl.ds(spin * count, count)],
            small_sem.at[place, spin],
        )
        for place, (target, pair_of) in enumerate(
            (
                (amp, (same_amp_ref, opposite_amp_ref)),
                (energy, (same_energy_ref, opposite_energy_ref)),
            )
        )
        for spin, source in enumerate(pair_of)
    ]
    for copy in small_copies:
        copy.start()
    for copy in small_copies:
        copy.wait()
    for step in range(1, AHEAD):
        begin(jnp.int32(step // parts), step % parts)
    share = jnp.where(lax.axis_index("pair") == 0, 1.0, 0.0)
    for pair in range(both):
        value = jnp.where(mask(ranks[pair], slots), amp[pair].astype(jnp.float32), 0.0)
        masked[pair] = value.astype(jnp.bfloat16)
        gaps = energy[pair]
        first = jnp.broadcast_to(gaps[0:1], (slots, slots)).T
        base_ref[pair] = (first + gaps[1:2]) * value * share
    total[...] = jnp.zeros_like(total)

    @pl.loop(0, both)
    def _(pair):
        settled = pair - (both - early)

        @pl.when(settled >= 0)
        def _():
            on_rows(ranks[settled], cuts, functools.partial(add_exchange, held, base_ref, settled))

        for part, (begins, length) in enumerate(spans):
            copies(same_ref, pair, part, lambda copy: copy.wait())
            begin(pair + (part + AHEAD) // parts, (part + AHEAD) % parts)

            def work(rows):
                for low, high in bounds[1:]:
                    if low >= rows - ROWS and high <= rows:

                        @pl.when(ranks[pair] <= low)
                        def _():
                            begin_at = slice(begins, begins + length)
                            held[pair, :, low:high, begin_at] = jnp.zeros(
                                (2, high - low, length), held.dtype
                            )

                weights = masked[pair, :rows, :rows]
                for at, size in pieces(length, STEP):
                    columns = slice(begins + at, begins + at + size)
                    left = held[pair, 0, :rows, columns]
                    right = held[pair, 1, :rows, columns]
                    mixed = jnp.dot(weights, right, preferred_element_type=jnp.float32)
                    dressed = left.astype(jnp.float32) * mixed
                    total[:, columns] += jnp.sum(dressed.reshape(rows // 8, 8, size), axis=0)

            on_rows(ranks[pair], cuts, work)


    coupling_ref[...] = jnp.sum(total[...], axis=0, keepdims=True)


def coulomb_kernel(same_ranks, opposite_ranks, held, base_ref, *rest, partners, group):
    couplings, outs = rest[:partners], rest[partners:-4]
    coupling, ranks, finished, whole = rest[-4:]
    both, _, slots, functions = held.shape
    count = both // 2
    aux_index = lax.axis_index("aux")
    start = aux_index * count
    for pair in range(count):
        ranks[pair] = same_ranks[start + pair]
        ranks[count + pair] = opposite_ranks[start + pair]
    coupling[...] = functools.reduce(jnp.add, [ref[...] for ref in couplings])
    finished[...] = jnp.zeros_like(finished)

    @pl.loop(0, both)
    def _(pair):
        def work(rows):
            summed = jnp.zeros((rows, rows), jnp.float32)
            for at, size in pieces(functions, STEP):
                columns = slice(at, at + size)
                left = held[pair, 0, :rows, columns].astype(jnp.float32)
                scaled = (left * coupling[:, columns]).astype(jnp.bfloat16)
                summed += lax.dot_general(
                    scaled,
                    held[pair, 1, :rows, columns],
                    ROW_BY_ROW,
                    preferred_element_type=jnp.float32,
                )
            finished[pair, :rows, :rows] = jnp.where(
                mask(ranks[pair], rows), summed + base_ref[pair, :rows, :rows], 0.0
            )

        on_rows(ranks[pair], row_cuts(slots), work)

    for pair in range(both):
        whole[:, pair, :] = finished[pair]
    rows = slots // len(outs)
    turn = lax.axis_index("pair") ^ lax.div(aux_index, group)
    for k, out in enumerate(outs):
        out[...] = whole[pl.ds((turn ^ k) * rows, rows)]


def add_kernel(held, *refs):
    refs[-1][...] = functools.reduce(jnp.add, [ref[...] for ref in refs[:-1]])


def gather_kernel(*refs, partners, group):
    parts, outs = refs[:partners], refs[partners:]
    rows = outs[0].shape[0]
    inner = lax.rem(lax.axis_index("aux"), group)
    for k, out in enumerate(outs):
        at = lax.rem(inner + k, group) * rows
        out[...] = functools.reduce(jnp.add, [ref[pl.ds(at, rows)] for ref in parts])


def last_kernel(*refs, group):
    parts, outs = refs[:group], refs[group:]
    count = parts[0].shape[1] // 2
    inner = lax.rem(lax.axis_index("aux"), group)
    values = [ref[...] for ref in parts]
    for j in range(group):
        value = values[0]
        for k in range(1, group):
            value = jnp.where(lax.rem(j + k, group) == inner, values[k], value)
        for spin, out in enumerate(outs):
            out[:, j * count : (j + 1) * count, :] = value[:, spin * count : (spin + 1) * count, :]


def body(
    same_panels,
    opposite_panels,
    same_amplitudes,
    opposite_amplitudes,
    same_energies,
    opposite_energies,
    same_ranks,
    opposite_ranks,
):
    count, _, slots, functions = same_panels.shape
    both = 2 * count
    pairs, auxes = lax.axis_size("pair"), lax.axis_size("aux")
    group = auxes // pairs
    rows = slots // auxes
    f32 = jnp.float32
    ranks = [(SCALARS, same_ranks), (SCALARS, opposite_ranks)]
    early = count + count // 2
    held, coupling, base = call(
        functools.partial(dressing_kernel, early=early),
        (
            ((both,) + same_panels.shape[1:], same_panels.dtype),
            ((1, functions), f32),
            ((both, slots, slots), f32),
        ),
        ranks
        + [
            (ANYWHERE, value)
            for value in (
                same_panels,
                opposite_panels,
                same_amplitudes,
                opposite_amplitudes,
                same_energies,
                opposite_energies,
            )
        ],
        [
            pltpu.VMEM((both, slots, slots), jnp.bfloat16),
            pltpu.VMEM((both, 2, slots), f32),
            pltpu.VMEM((both, slots, slots), jnp.bfloat16),
            pltpu.VMEM((8, functions), f32),
            pltpu.SMEM((both,), jnp.int32),
            pltpu.SemaphoreType.DMA((both, len(column_spans(functions)), len(copy_bounds(slots)))),
            pltpu.SemaphoreType.DMA((2, 2)),
        ],
        flops=8 * count * slots * slots * functions,
        name="dressing",
    )

    def swapped(value, k):
        return lax.ppermute(value, "aux", [(i, i ^ k) for i in range(auxes)])

    (coupling,) = call(
        add_kernel,
        (((1, functions), f32),),
        [(ON_CHIP, value) for value in (held, coupling, swapped(coupling, 1))],
        name="chip_sum",
    )
    couplings = [coupling] + [swapped(coupling, k) for k in range(2, auxes, 2)]
    (base,) = call(
        functools.partial(exchange_kernel, early=early),
        (((both, slots, slots), f32),),
        ranks + [(ON_CHIP, held), (ON_CHIP, base)],
        [pltpu.SMEM((both,), jnp.int32)],
        flops=2 * (both - early) * slots * slots * functions,
        name="exchange",
    )
    leaving = call(
        functools.partial(coulomb_kernel, partners=len(couplings), group=group),
        (((group * rows, both, slots), f32),) * pairs,
        ranks + [(ON_CHIP, value) for value in (held, base, *couplings)],
        [
            pltpu.VMEM((1, functions), f32),
            pltpu.SMEM((both,), jnp.int32),
            pltpu.VMEM((both, slots, slots), f32),
            pltpu.VMEM((slots, both, slots), f32),
        ],
        flops=4 * count * slots * slots * functions,
        name="coulomb",
    )
    parts = [leaving[0]] + [
        lax.ppermute(leaving[k], "pair", [(i, i ^ k) for i in range(pairs)])
        for k in range(1, pairs)
    ]
    moving = call(
        functools.partial(gather_kernel, partners=pairs, group=group),
        (((rows, both, slots), f32),) * group,
        [(ON_CHIP, value) for value in parts],
        name="pair_sum",
    )
    arrived = []
    for k in range(group):
        moves = [
            (
                p * auxes + q,
                (q // group) * auxes
                + group * (p ^ (q // group))
                + (q % group + k) % group,
            )
            for p in range(pairs)
            for q in range(auxes)
        ]
        arrived.append(lax.ppermute(moving[k], ("pair", "aux"), moves))
    outs = pl.pallas_call(
        functools.partial(last_kernel, group=group),
        out_shape=(jax.ShapeDtypeStruct((rows, group * count, slots), f32),) * 2,
        in_specs=[ON_CHIP] * group,
        out_specs=(ON_CHIP, ON_CHIP),
        name="residual_rows",
    )(*(pltpu.with_memory_space_constraint(value, pltpu.VMEM) for value in arrived))
    return tuple(out.transpose(1, 0, 2) for out in outs)


def solution(mesh):
    placed = (
        P("aux", None, None, "pair"),
        P("aux", None, None, "pair"),
        P(),
        P(),
        P(),
        P(),
        P(),
        P(),
    )
    return jax.shard_map(
        body,
        mesh=mesh,
        in_specs=placed,
        out_specs=(P("pair", "aux", None), P("pair", "aux", None)),
        check_vma=False,
    )
```

```python
import functools

import jax
import jax.numpy as jnp
from jax import lax
from jax.experimental import pallas as pl
from jax.experimental.pallas import tpu as pltpu
from jax.sharding import PartitionSpec as P

STEP = 256
AHEAD = 3
PARTS = 1
LANES = 128
ROWS = 16
SMALL = 8 * 1024 * 1024
ROW_BY_ROW = (((1,), (1,)), ((), ()))

ANYWHERE = pl.BlockSpec(memory_space=pltpu.HBM)
SCALARS = pl.BlockSpec(memory_space=pltpu.SMEM)
ON_CHIP = pl.BlockSpec(memory_space=pltpu.VMEM)


def pieces(total, step):
    return [(at, min(step, total - at)) for at in range(0, total, step)]


def column_spans(functions):
    if functions % LANES:
        return [(0, functions)]
    length = -(-functions // (PARTS * STEP)) * STEP
    return pieces(functions, length)


def call(kernel, outs, ins, scratch=(), flops=0, name=None):
    placed = [
        value if spec is not ON_CHIP else pltpu.with_memory_space_constraint(value, pltpu.VMEM)
        for spec, value in ins
    ]
    return pl.pallas_call(
        kernel,
        out_shape=tuple(pltpu.VMEM(shape, dtype) for shape, dtype in outs),
        in_specs=[spec for spec, _ in ins],
        out_specs=(ON_CHIP,) * len(outs),
        scratch_shapes=list(scratch),
        compiler_params=pltpu.CompilerParams(vmem_limit_bytes=SMALL),
        cost_estimate=pl.CostEstimate(flops=flops, bytes_accessed=0, transcendentals=0),
        name=name,
    )(*placed)


def mask(rank, slots):
    rows = lax.broadcasted_iota(jnp.int32, (slots, slots), 0) < rank
    columns = lax.broadcasted_iota(jnp.int32, (slots, slots), 1) < rank
    return jnp.logical_and(rows, columns)


def row_cuts(slots):
    least = slots * 3 // 7 // ROWS * ROWS
    return list(range(least, slots, ROWS)) + [slots] if least else [slots]


def on_rows(rank, cuts, work):
    for place, rows in enumerate(cuts):
        fits = rank <= rows
        if place == len(cuts) - 1:
            fits = True
        if place:
            fits = jnp.logical_and(rank > cuts[place - 1], fits)
        pl.when(fits)(functools.partial(work, rows))


def add_exchange(held, base_ref, pair, rows):
    exchange = jnp.zeros((rows, rows), jnp.float32)
    for at, size in pieces(held.shape[-1], STEP):
        exchange += lax.dot_general(
            held[pair, 0, :rows, at : at + size],
            held[pair, 1, :rows, at : at + size],
            ROW_BY_ROW,
            preferred_element_type=jnp.float32,
        )
    base_ref[pair, :rows, :rows] += exchange


def exchange_kernel(same_ranks, opposite_ranks, held, base_in, base_ref, ranks, *, early):
    both, _, slots, _ = held.shape
    count = both // 2
    start = lax.axis_index("aux") * count
    for pair in range(count):
        ranks[pair] = same_ranks[start + pair]
        ranks[count + pair] = opposite_ranks[start + pair]
    base_ref[...] = base_in[...]

    @pl.loop(early, both)
    def _(pair):
        on_rows(
            ranks[pair], row_cuts(slots), functools.partial(add_exchange, held, base_ref, pair)
        )


def dressing_kernel(
    same_ranks,
    opposite_ranks,
    same_ref,
    opposite_ref,
    same_amp_ref,
    opposite_amp_ref,
    same_energy_ref,
    opposite_energy_ref,
    held,
    coupling_ref,
    base_ref,
    amp,
    energy,
    masked,
    total,
    ranks,
    panel_sem,
    small_sem,
    *,
    early,
):
    both, _, slots, functions = held.shape
    count = both // 2
    start = lax.axis_index("aux") * count
    sources = (same_ref, opposite_ref)
    cuts = row_cuts(slots)
    bounds = list(zip([0] + cuts[:-1], cuts))
    spans = column_spans(functions)
    parts = len(spans)
    for pair in range(count):
        ranks[pair] = same_ranks[start + pair]
        ranks[count + pair] = opposite_ranks[start + pair]

    def copies(source, pair, part, do):
        at, size = spans[part]
        for place, (low, high) in enumerate(bounds):

            def one(place=place, low=low, high=high):
                do(
                    pltpu.make_async_copy(
                        source.at[lax.rem(pair, count), :, low:high, pl.ds(at, size)],
                        held.at[pair, :, low:high, pl.ds(at, size)],
                        panel_sem.at[pair, part, place],
                    )
                )

            if place:
                pl.when(ranks[pair] > low)(one)
            else:
                one()

    def begin(pair, part):
        for spin, source in enumerate(sources):

            @pl.when(jnp.logical_and(pair >= spin * count, pair < (spin + 1) * count))
            def _():
                copies(source, pair, part, lambda copy: copy.start())

    begin(jnp.int32(0), 0)
    small_copies = [
        pltpu.make_async_copy(
            source.at[pl.ds(start, count)],
            target.at[pl.ds(spin * count, count)],
            small_sem.at[place, spin],
        )
        for place, (target, pair_of) in enumerate(
            (
                (amp, (same_amp_ref, opposite_amp_ref)),
                (energy, (same_energy_ref, opposite_energy_ref)),
            )
        )
        for spin, source in enumerate(pair_of)
    ]
    for copy in small_copies:
        copy.start()
    for copy in small_copies:
        copy.wait()
    for step in range(1, AHEAD):
        begin(jnp.int32(step // parts), step % parts)
    share = jnp.where(lax.axis_index("pair") == 0, 1.0, 0.0)
    for pair in range(both):
        value = jnp.where(mask(ranks[pair], slots), amp[pair].astype(jnp.float32), 0.0)
        masked[pair] = value.astype(jnp.bfloat16)
        gaps = energy[pair]
        first = jnp.broadcast_to(gaps[0:1], (slots, slots)).T
        base_ref[pair] = (first + gaps[1:2]) * value * share
    total[...] = jnp.zeros_like(total)

    @pl.loop(0, both)
    def _(pair):
        settled = pair - (both - early)

        @pl.when(settled >= 0)
        def _():
            on_rows(ranks[settled], cuts, functools.partial(add_exchange, held, base_ref, settled))

        for part, (begins, length) in enumerate(spans):
            copies(same_ref, pair, part, lambda copy: copy.wait())
            begin(pair + (part + AHEAD) // parts, (part + AHEAD) % parts)

            def work(rows):
                weights = masked[pair, :rows, :rows]
                for at, size in pieces(length, STEP):
                    columns = slice(begins + at, begins + at + size)
                    left = held[pair, 0, :rows, columns]
                    right = held[pair, 1, :rows, columns]
                    mixed = jnp.dot(weights, right, preferred_element_type=jnp.float32)
                    dressed = left.astype(jnp.float32) * mixed
                    total[:, columns] += jnp.sum(dressed.reshape(rows // 8, 8, size), axis=0)

            on_rows(ranks[pair], cuts, work)


    coupling_ref[...] = jnp.sum(total[...], axis=0, keepdims=True)


def coulomb_kernel(same_ranks, opposite_ranks, held, base_ref, *rest, partners, group):
    couplings, outs = rest[:partners], rest[partners:-4]
    coupling, ranks, finished, whole = rest[-4:]
    both, _, slots, functions = held.shape
    count = both // 2
    aux_index = lax.axis_index("aux")
    start = aux_index * count
    for pair in range(count):
        ranks[pair] = same_ranks[start + pair]
        ranks[count + pair] = opposite_ranks[start + pair]
    coupling[...] = functools.reduce(jnp.add, [ref[...] for ref in couplings])
    finished[...] = jnp.zeros_like(finished)

    @pl.loop(0, both)
    def _(pair):
        def work(rows):
            summed = jnp.zeros((rows, rows), jnp.float32)
            for at, size in pieces(functions, STEP):
                columns = slice(at, at + size)
                left = held[pair, 0, :rows, columns].astype(jnp.float32)
                scaled = (left * coupling[:, columns]).astype(jnp.bfloat16)
                summed += lax.dot_general(
                    scaled,
                    held[pair, 1, :rows, columns],
                    ROW_BY_ROW,
                    preferred_element_type=jnp.float32,
                )
            finished[pair, :rows, :rows] = jnp.where(
                mask(ranks[pair], rows), summed + base_ref[pair, :rows, :rows], 0.0
            )

        on_rows(ranks[pair], row_cuts(slots), work)

    for pair in range(both):
        whole[:, pair, :] = finished[pair]
    rows = slots // len(outs)
    turn = row_owner(lax.axis_index("pair"), lax.div(aux_index, group), len(outs))
    for k, out in enumerate(outs):
        out[...] = whole[pl.ds((turn ^ k) * rows, rows)]


def row_owner(pair, owner, pairs):
    return pair ^ owner ^ (pairs - 1) * (1 - 2 * owner // pairs)


def add_kernel(held, *refs):
    refs[-1][...] = functools.reduce(jnp.add, [ref[...] for ref in refs[:-1]])


def gather_kernel(*refs, partners, group):
    parts, outs = refs[:partners], refs[partners:]
    rows = outs[0].shape[0]
    inner = lax.rem(lax.axis_index("aux"), group)
    for k, out in enumerate(outs):
        at = lax.rem(inner + k, group) * rows
        out[...] = functools.reduce(jnp.add, [ref[pl.ds(at, rows)] for ref in parts])


def last_kernel(*refs, group):
    parts, outs = refs[:group], refs[group:]
    count = parts[0].shape[1] // 2
    inner = lax.rem(lax.axis_index("aux"), group)
    values = [ref[...] for ref in parts]
    for j in range(group):
        value = values[0]
        for k in range(1, group):
            value = jnp.where(lax.rem(j + k, group) == inner, values[k], value)
        for spin, out in enumerate(outs):
            out[:, j * count : (j + 1) * count, :] = value[:, spin * count : (spin + 1) * count, :]


def body(
    same_panels,
    opposite_panels,
    same_amplitudes,
    opposite_amplitudes,
    same_energies,
    opposite_energies,
    same_ranks,
    opposite_ranks,
):
    count, _, slots, functions = same_panels.shape
    both = 2 * count
    pairs, auxes = lax.axis_size("pair"), lax.axis_size("aux")
    group = auxes // pairs
    rows = slots // auxes
    f32 = jnp.float32
    ranks = [(SCALARS, same_ranks), (SCALARS, opposite_ranks)]
    early = count + count // 4
    held, coupling, base = call(
        functools.partial(dressing_kernel, early=early),
        (
            ((both,) + same_panels.shape[1:], same_panels.dtype),
            ((1, functions), f32),
            ((both, slots, slots), f32),
        ),
        ranks
        + [
            (ANYWHERE, value)
            for value in (
                same_panels,
                opposite_panels,
                same_amplitudes,
                opposite_amplitudes,
                same_energies,
                opposite_energies,
            )
        ],
        [
            pltpu.VMEM((both, slots, slots), jnp.bfloat16),
            pltpu.VMEM((both, 2, slots), f32),
            pltpu.VMEM((both, slots, slots), jnp.bfloat16),
            pltpu.VMEM((8, functions), f32),
            pltpu.SMEM((both,), jnp.int32),
            pltpu.SemaphoreType.DMA((both, len(column_spans(functions)), len(row_cuts(slots)))),
            pltpu.SemaphoreType.DMA((2, 2)),
        ],
        flops=8 * count * slots * slots * functions,
        name="dressing",
    )

    def swapped(value, k):
        return lax.ppermute(value, "aux", [(i, i ^ k) for i in range(auxes)])

    (coupling,) = call(
        add_kernel,
        (((1, functions), f32),),
        [(ON_CHIP, value) for value in (held, coupling, swapped(coupling, 1))],
        name="chip_sum",
    )
    couplings = [coupling] + [swapped(coupling, k) for k in range(2, auxes, 2)]
    (base,) = call(
        functools.partial(exchange_kernel, early=early),
        (((both, slots, slots), f32),),
        ranks + [(ON_CHIP, held), (ON_CHIP, base)],
        [pltpu.SMEM((both,), jnp.int32)],
        flops=2 * (both - early) * slots * slots * functions,
        name="exchange",
    )
    leaving = call(
        functools.partial(coulomb_kernel, partners=len(couplings), group=group),
        (((group * rows, both, slots), f32),) * pairs,
        ranks + [(ON_CHIP, value) for value in (held, base, *couplings)],
        [
            pltpu.VMEM((1, functions), f32),
            pltpu.SMEM((both,), jnp.int32),
            pltpu.VMEM((both, slots, slots), f32),
            pltpu.VMEM((slots, both, slots), f32),
        ],
        flops=4 * count * slots * slots * functions,
        name="coulomb",
    )
    parts = [leaving[0]] + [
        lax.ppermute(leaving[k], "pair", [(i, i ^ k) for i in range(pairs)])
        for k in range(1, pairs)
    ]
    moving = call(
        functools.partial(gather_kernel, partners=pairs, group=group),
        (((rows, both, slots), f32),) * group,
        [(ON_CHIP, value) for value in parts],
        name="pair_sum",
    )
    arrived = []
    for k in range(group):
        moves = [
            (
                p * auxes + q,
                (q // group) * auxes
                + group * row_owner(p, q // group, pairs)
                + (q % group + k) % group,
            )
            for p in range(pairs)
            for q in range(auxes)
        ]
        arrived.append(lax.ppermute(moving[k], ("pair", "aux"), moves))
    outs = pl.pallas_call(
        functools.partial(last_kernel, group=group),
        out_shape=(jax.ShapeDtypeStruct((rows, group * count, slots), f32),) * 2,
        in_specs=[ON_CHIP] * group,
        out_specs=(ON_CHIP, ON_CHIP),
        name="residual_rows",
    )(*(pltpu.with_memory_space_constraint(value, pltpu.VMEM) for value in arrived))
    return tuple(out.transpose(1, 0, 2) for out in outs)


def solution(mesh):
    placed = (
        P("aux", None, None, "pair"),
        P("aux", None, None, "pair"),
        P(),
        P(),
        P(),
        P(),
        P(),
        P(),
    )
    return jax.shard_map(
        body,
        mesh=mesh,
        in_specs=placed,
        out_specs=(P("pair", "aux", None), P("pair", "aux", None)),
        check_vma=False,
    )
```
